32 devices in a mesh: blk: 8 (over y, x, core), grp: 4 (over z).
Axes of the slice: x: 2, y: 2, z: 4, core: 2. Of those that a mesh axis runs over, the one named last changes fastest.
Arguments:
- images: bfloat16 [12288, 1152], P(('blk', 'grp')), may hold values from -0.71875 to 0.71875
- texts: bfloat16 [12288, 1152], P(('blk', 'grp')), may hold values from -0.71875 to 0.71875
- text_exps: int32 [96], P(('blk', 'grp')), may hold values from -1 to 1
- counts: int32 [32], P(('blk', 'grp')), may hold values from 128 to 384, as said below
- log_temp: float32 [1], replicated, may hold values from 1.1 to 2.3
- bias: float32 [1], replicated, may hold values from -6 to -4
Outputs:
- image_grad: float32 [12288, 1152], P(('blk', 'grp'))
- text_grad: float32 [12288, 1152], P(('blk', 'grp'))
- row_loss: float32 [12288], P(('blk', 'grp'))
- scalar_grads: float32 [2], replicated
The draws below stay inside these ranges and needn't reach their ends.
Inputs may be any that keep to these rules, and one draw needn't show every extreme that they name: `counts`: each device's count lies between 128 and 384; some device has all 384 rows valid.
All inputs are finite; a program needn't handle non-finite values.
Results may differ from the reference program's by a relative error of at most 0.0095.
Values may be sent and summed in bfloat16 or wider, within the bound.
A program may use at most 128 MiB of HBM per device.

```python
import jax
import jax.numpy as jnp
from jax import lax

D = 1152
ROWS_DEV = 384
SPAN = 128
STEPS = 2
TOKENS = 12288
N_BLK = 8
N_GRP = 4


def draw_counts(key, part):
    total = N_BLK * N_GRP
    values = jax.random.randint(key, (total,), ROWS_DEV // 3, ROWS_DEV + 1).astype(jnp.int32)
    where_full = jax.random.randint(jax.random.fold_in(key, 7), (), 0, total)
    return values.at[where_full].set(ROWS_DEV).astype(jnp.int32)


def with_ends(drawn, stream_key, least, top_value):
    longest = drawn.shape.index(max(drawn.shape))
    spots = []
    for shift in (0, 1):
        where = [jax.random.randint(jax.random.fold_in(stream_key, axis), (), 0, length) for axis, length in enumerate(drawn.shape)]
        where[longest] = (where[longest] + shift) % drawn.shape[longest]
        spots.append(tuple(where))
    return drawn.at[spots[0]].set(least).at[spots[1]].set(top_value)


def shard_levels(rng, dims, split, smallest, largest):
    level, own = 1.0, jax.random.fold_in(rng, 6)
    for position, shards_of in split:
        steps = jnp.exp(jax.random.uniform(jax.random.fold_in(own, position), (shards_of,), jnp.float32, smallest / len(split), largest / len(split)))
        level = level * jnp.repeat(steps, dims[position] // shards_of).reshape([-1 if axis == position else 1 for axis in range(len(dims))])
    return level


def scatter_about(rng, dims, spread, most, pieces=(), kind=jnp.bfloat16):
    array = jax.random.normal(rng, dims, jnp.float32) * spread
    if len(pieces) > 0:
        array = shard_levels(rng, dims, pieces, -0.22, 0.18) * array
    return jnp.clip(array, min=-most, max=most).astype(kind)


def setup_inputs(seed: int = 0) -> dict:
    keys = jax.random.split(jax.random.key(seed), 7)
    return {
        "images": scatter_about(keys[0], (TOKENS, D), 0.12, 0.71875, ((0, 32),)),
        "texts": scatter_about(keys[1], (TOKENS, D), 0.12, 0.71875, ((0, 32),)),
        "text_exps": with_ends(jax.random.randint(keys[2], (TOKENS // SPAN,), -1, 2), jax.random.fold_in(keys[2], 1), -1, 1).astype(jnp.int32),
        "counts": draw_counts(jax.random.fold_in(keys[6], 71), 0),
        "log_temp": jnp.clip(jax.random.uniform(keys[4], (1,), jnp.float32, 1.1, 2.3), 1.1, 2.3),
        "bias": jnp.clip(jax.random.uniform(keys[5], (1,), jnp.float32, -6.0, -4.0), -6.0, -4.0),
    }


def reference(images, texts, text_exps, counts, log_temp, bias):
    groups = N_GRP
    loops = N_BLK
    GR = groups * ROWS_DEV
    temp = jnp.exp(log_temp[0])
    shift_b = bias[0]
    scale = jnp.exp2(text_exps.astype(jnp.float32))
    scaled = (texts.astype(jnp.float32).reshape(-1, SPAN, D) * scale[:, None, None]).reshape(TOKENS, D).astype(jnp.bfloat16)
    valid = (jnp.arange(ROWS_DEV)[None, :] < counts[:, None]).reshape(loops, GR)
    image_groups = images.reshape(loops, GR, D)
    text_groups = scaled.reshape(loops, GR, D)
    match = jnp.arange(GR)[:, None] == jnp.arange(GR)[None, :]
    row_loss = jnp.zeros((loops, GR), jnp.float32)
    image_grad = jnp.zeros((loops, GR, D), jnp.float32)
    text_grad = jnp.zeros((loops, GR, D), jnp.float32)
    sum_temp = jnp.zeros((), jnp.float32)
    sum_bias = jnp.zeros((), jnp.float32)
    for step in range(STEPS):
        def one_group(bidx):
            other = (bidx - step) % loops
            xmat = image_groups[bidx]
            ymat = text_groups[other]
            mask = valid[bidx][:, None] & valid[other][None, :]
            scores = jnp.dot(xmat, ymat.T, preferred_element_type=jnp.float32)
            logits = temp * scores + shift_b
            if step == 0:
                sign = jnp.where(match, 1.0, -1.0).astype(jnp.float32)
            else:
                sign = -jnp.ones((GR, GR), jnp.float32)
            loss = jnp.sum(jnp.where(mask, jax.nn.softplus(-sign * logits), 0.0), axis=1)
            dlogit = jnp.where(mask, -sign * jax.nn.sigmoid(-sign * logits), 0.0)
            dround = dlogit.astype(jnp.bfloat16)
            dx = temp * jnp.dot(dround, ymat, preferred_element_type=jnp.float32)
            parts = jnp.einsum("grj,grd->gjd", dround.reshape(groups, ROWS_DEV, GR).astype(jnp.float32), xmat.reshape(groups, ROWS_DEV, D).astype(jnp.float32), precision=lax.Precision.HIGHEST)
            parts = (temp * parts).astype(jnp.bfloat16).astype(jnp.float32)
            part = jnp.sum(parts, axis=0)
            return loss, dx, part, jnp.sum(dlogit * temp * scores), jnp.sum(dlogit)
        loss, dx, part, st, sb = lax.map(one_group, jnp.arange(loops, dtype=jnp.int32))
        row_loss = row_loss + loss
        image_grad = image_grad + dx
        text_grad = text_grad + jnp.roll(part, -step, axis=0)
        sum_temp = sum_temp + jnp.sum(st)
        sum_bias = sum_bias + jnp.sum(sb)
    return (image_grad.reshape(TOKENS, D), text_grad.reshape(TOKENS, D), row_loss.reshape(TOKENS), jnp.stack([sum_temp, sum_bias]))
```

```python
import functools

import jax
import jax.numpy as jnp
from jax import lax
from jax.experimental import pallas as pl
from jax.experimental.pallas import tpu as pltpu
from jax.sharding import PartitionSpec as P

MESH = pl.DeviceIdType.MESH
SPAN = 128
F32 = jnp.float32
BF16 = jnp.bfloat16


def kernel(
    B, G, C,
    scal, img, ivalid, txt, tmask,
    ig, tg, loss, sums,
    T, AQ, R, RX, M, acc, sz, sb,
    load_sem, agS, agR, xS, xR, qS, qR, rS, rR, mS, mR, szS, szR, sbS, sbR,
):
    b = lax.axis_index("blk")
    z = lax.axis_index("grp")
    rows = img.shape[0]
    nxt = lax.rem(b + 1, B)
    prv = lax.rem(b + B - 1, B)
    up = jnp.minimum(z + 1, G - 1)
    down = jnp.maximum(z - 1, 0)
    temp = scal[0]
    bias = scal[1]

    def remote(src, dst, ss, rs, dev):
        return pltpu.make_async_remote_copy(
            src_ref=src, dst_ref=dst, send_sem=ss, recv_sem=rs, device_id=dev, device_id_type=MESH
        )

    load = pltpu.make_async_copy(txt, T.at[z], load_sem)
    load.start()
    load_m = pltpu.make_async_copy(tmask, M.at[z], mR.at[0, z])
    load_m.start()

    bar = pltpu.get_barrier_semaphore()
    partners = 0
    for d in range(1, G):
        pl.semaphore_signal(bar, inc=1, device_id=(b, lax.rem(z + d, G)), device_id_type=MESH)
        partners += 1
    for d in range(1, B):
        other = lax.rem(b + d, B)
        for e in range(G if d in (1, B - 1) else 1):
            pl.semaphore_signal(bar, inc=1, device_id=(other, lax.rem(z + e, G)), device_id_type=MESH)
            partners += 1

    ig[...] = jnp.zeros_like(ig)
    loss[...] = jnp.zeros_like(loss)
    acc[...] = jnp.zeros_like(acc)
    load.wait()
    load_m.wait()
    pl.semaphore_wait(bar, partners)

    def ag(zt, c, direction):
        return remote(T.at[zt, c], T.at[zt, c], agS.at[direction, zt, c], agR.at[zt, c],
                      (b, up if direction == 0 else down))

    def xs(zt, c):
        return remote(T.at[zt, c], T.at[G + zt, c], xS.at[zt, c], xR.at[zt, c], (nxt, z))

    def qs(zt, c):
        return remote(AQ.at[G + zt, c], R.at[zt, c], qS.at[zt, c], qR.at[zt, c], (prv, z))

    def rs(zt, c, slot, direction):
        return remote(AQ.at[zt, c], RX.at[slot, c], rS.at[zt, c], rR.at[slot, c],
                      (b, up if direction == 0 else down))

    def mask_copies():
        copies = []
        for d in range(1, G):
            copies.append(remote(tmask, M.at[z], mS.at[0, d], mR.at[0, z], (b, lax.rem(z + d, G))))
        for e in range(G):
            copies.append(remote(tmask, M.at[G + z], mS.at[1, e], mR.at[1, z], (nxt, lax.rem(z + e, G))))
        return copies

    def scalar_z(d):
        return remote(acc, sz.at[z], szS.at[d], szR.at[z], (b, lax.rem(z + d, G)))

    def scalar_b(d):
        return remote(sz.at[G], sb.at[b], sbS.at[d], sbR.at[b], (lax.rem(b + d, B), z))

    masks = mask_copies()

    def item(t, kind):
        if kind == 2:
            return (t >= 0) & (t < C), jnp.clip(t, 0, C - 1), z
        n = G - 1 - z if kind == 0 else z
        safe = jnp.maximum(n, 1)
        j = t - 1
        valid = (j >= 0) & (j < C * n)
        j = jnp.clip(j, 0, C * safe - 1)
        c = lax.div(j, safe)
        off = 1 + lax.rem(j, safe)
        zt = z + off if kind == 0 else z - off
        return valid, c, jnp.clip(zt, 0, G - 1)

    def tile(step, zt, c):
        block = T[step * G + zt, c]
        scores = lax.dot_general(
            img[...], block, (((1,), (1,)), ((), ())), preferred_element_type=F32
        )
        logits = temp * scores + bias
        row = lax.broadcasted_iota(jnp.int32, (rows, SPAN), 0)
        col = lax.broadcasted_iota(jnp.int32, (rows, SPAN), 1)
        shift = (zt - z) * rows + c * SPAN + step * (G * rows * 2)
        x = jnp.where(col + shift == row, -logits, logits)
        flip = jnp.where(col + shift == row, -1.0, 1.0)
        e = jnp.exp(-jnp.abs(x))
        mask = ivalid[...] * M[step * G + zt, c][0:1, :]
        on = mask > 0.5
        soft = jnp.maximum(x, 0.0) + jnp.log1p(e)
        sig = jnp.where(x >= 0, 1.0, e) / (1.0 + e)
        dlogit = jnp.where(on, flip * sig, 0.0)
        loss[...] += jnp.where(on, soft, 0.0)
        prod = dlogit * (temp * scores)
        acc[0:8, :] += jnp.sum(prod.reshape(rows // 8, 8, SPAN), axis=0)
        acc[8:16, :] += jnp.sum(dlogit.reshape(rows // 8, 8, SPAN), axis=0)
        dround = dlogit.astype(BF16)
        ig[...] += jnp.dot(dround, block, preferred_element_type=F32)
        part = lax.dot_general(
            dround, img[...], (((0,), (0,)), ((), ())), preferred_element_type=F32
        )
        AQ[step * G + zt, c] = (temp * part).astype(BF16)

    jobs_end = C * (G - 1) + 2
    slots = C * (G - 1) + G + 2

    def slot(t, carry):
        for direction in (0, 1):
            n = z + 1 if direction == 0 else G - z
            c = lax.div(t, n)
            edge = z < G - 1 if direction == 0 else z > 0
            due = edge & (lax.rem(t, n) == 0) & (c < C)

            @pl.when(due)
            def _():
                ag(z, jnp.minimum(c, C - 1), direction).start()

        for kind in (0, 1, 2):
            valid, c, zt = item(t, kind)

            @pl.when(valid)
            def _():
                if kind != 2:
                    onward = 1 if kind == 0 else 0
                    ag(zt, c, onward).wait_recv()

                    @pl.when(z > 0 if kind == 0 else z < G - 1)
                    def _():
                        ag(zt, c, onward).start()

                xs(zt, c).start()

        @pl.when(t == 0)
        def _():
            for copy in masks:
                copy.start()
            for d in range(1, G):
                other = lax.rem(z + d, G)
                remote(tmask, M.at[other], mS.at[0, d], mR.at[0, other], (b, other)).wait_recv()
            for e in range(G):
                other = lax.rem(z + e, G)
                remote(tmask, M.at[G + other], mS.at[1, e], mR.at[1, other], (nxt, other)).wait_recv()

        def job(k, carry):
            step = 1 - lax.div(k, 3)
            kind = lax.rem(k, 3)
            tt = t - step
            v0, c0, z0 = item(tt, 0)
            v1, c1, z1 = item(tt, 1)
            v2, c2, z2 = item(tt, 2)
            c = jnp.where(kind == 0, c0, jnp.where(kind == 1, c1, c2))
            zt = jnp.where(kind == 0, z0, jnp.where(kind == 1, z1, z2))
            valid = ((kind == 0) & v0) | ((kind == 1) & v1) | ((kind == 2) & v2)

            @pl.when(valid)
            def _():
                @pl.when(step == 1)
                def _():
                    xs(zt, c).wait_recv()

                tile(step, zt, c)

                @pl.when(step == 1)
                def _():
                    qs(zt, c).start()

            return carry

        @pl.when(t < jobs_end)
        def _():
            lax.fori_loop(0, 6, job, 0)

        @pl.when((t >= 2) & (t < C + 2))
        def _():
            c = jnp.clip(t - 2, 0, C - 1)
            qs(z, c).wait_recv()
            tg[c] = AQ[z, c].astype(F32) + R[z, c].astype(F32)

        for direction in (0, 1):
            far = z if direction == 0 else G - 1 - z
            v = t - 3 - far
            vc = jnp.clip(v, 0, C * (G - 1) - 1)
            c = lax.div(vc, G - 1)
            target = lax.rem(vc, G - 1) + 1
            zt = target if direction == 0 else G - 1 - target
            live = (v >= 0) & (v < C * (G - 1)) & (target >= far)

            @pl.when(live & (target > far))
            def _():
                qs(zt, c).wait_recv()

                @pl.when(far == 0)
                def _():
                    AQ[zt, c] = (AQ[zt, c].astype(F32) + R[zt, c].astype(F32)).astype(BF16)

                @pl.when(far > 0)
                def _():
                    rs(zt, c, zt, direction).wait_recv()
                    AQ[zt, c] = (
                        AQ[zt, c].astype(F32) + R[zt, c].astype(F32) + RX[zt, c].astype(F32)
                    ).astype(BF16)

                last = target == far + 1
                where = jnp.where(last & (direction == 1), G, zt)
                rs(zt, c, where, direction).start()

            @pl.when(live & (target == far))
            def _():
                place = z if direction == 0 else G
                rs(zt, c, place, direction).wait_recv()
                tg[c] = tg[c] + RX[place, c].astype(F32)

        @pl.when(t == jobs_end)
        def _():
            for d in range(1, G):
                scalar_z(d).start()
            sz[z] = acc[...]

        @pl.when(t == jobs_end + 1)
        def _():
            for d in range(1, G):
                other = lax.rem(z + d, G)
                remote(acc, sz.at[other], szS.at[d], szR.at[other], (b, other)).wait_recv()
            total = sz[0]
            for g in range(1, G):
                total = total + sz[g]
            sz[G] = total
            sb[b] = total
            for d in range(1, B):
                scalar_b(d).start()

        return carry

    lax.fori_loop(0, slots, slot, 0)

    for d in range(1, B):
        other = lax.rem(b + d, B)
        remote(sz.at[G], sb.at[other], sbS.at[d], sbR.at[other], (other, z)).wait_recv()
    total = sb[0]
    for g in range(1, B):
        total = total + sb[g]
    sums[...] = total
    ig[...] = ig[...] * temp

    for copy in masks:
        copy.wait_send()
    for d in range(1, G):
        scalar_z(d).wait_send()
    for d in range(1, B):
        scalar_b(d).wait_send()

    def drain(i, carry):
        zt, c = lax.div(i, C), lax.rem(i, C)
        xs(zt, c).wait_send()
        qs(zt, c).wait_send()

        @pl.when(zt != z)
        def _():
            rs(zt, c, zt, 0).wait_send()

        @pl.when((zt <= z) & (z < G - 1))
        def _():
            ag(zt, c, 0).wait_send()

        @pl.when((zt >= z) & (z > 0))
        def _():
            ag(zt, c, 1).wait_send()

        return carry

    lax.fori_loop(0, G * C, drain, 0)


def on_device(B, G, images, texts, text_exps, counts, log_temp, bias):
    rows, width = images.shape
    C = rows // SPAN
    scale = jnp.exp2(text_exps.astype(F32))
    scaled = (texts.astype(F32).reshape(C, SPAN, width) * scale[:, None, None]).astype(BF16)
    scal = jnp.concatenate([jnp.exp(log_temp), bias])
    ivalid = jnp.broadcast_to(
        (jnp.arange(rows)[:, None] < counts[0]).astype(F32), (rows, SPAN)
    )
    tmask = jnp.broadcast_to(
        (jnp.arange(rows) < counts[0]).astype(F32).reshape(C, 1, SPAN), (C, 8, SPAN)
    )
    vmem = pl.BlockSpec(memory_space=pltpu.VMEM)
    hbm = pl.BlockSpec(memory_space=pl.ANY)
    dma = pltpu.SemaphoreType.DMA
    flops = 2 * G * 3 * 2 * rows * rows * width
    ig, tg, loss, sums = pl.pallas_call(
        functools.partial(kernel, B, G, C),
        out_shape=(
            jax.ShapeDtypeStruct((rows, width), F32),
            jax.ShapeDtypeStruct((C, SPAN, width), F32),
            jax.ShapeDtypeStruct((rows, SPAN), F32),
            jax.ShapeDtypeStruct((16, SPAN), F32),
        ),
        in_specs=[pl.BlockSpec(memory_space=pltpu.SMEM), vmem, vmem, hbm, vmem],
        out_specs=(vmem, vmem, vmem, vmem),
        scratch_shapes=[
            pltpu.VMEM((2 * G, C, SPAN, width), BF16),
            pltpu.VMEM((2 * G, C, SPAN, width), BF16),
            pltpu.VMEM((G, C, SPAN, width), BF16),
            pltpu.VMEM((G + 1, C, SPAN, width), BF16),
            pltpu.VMEM((2 * G, C, 8, SPAN), F32),
            pltpu.VMEM((16, SPAN), F32),
            pltpu.VMEM((G + 1, 16, SPAN), F32),
            pltpu.VMEM((B, 16, SPAN), F32),
            dma(()),
            dma((2, G, C)), dma((G, C)),
            dma((G, C)), dma((G, C)),
            dma((G, C)), dma((G, C)),
            dma((G, C)), dma((G + 1, C)),
            dma((2, G)), dma((2, G)),
            dma((G,)), dma((G,)),
            dma((B,)), dma((B,)),
        ],
        compiler_params=pltpu.CompilerParams(
            collective_id=0, has_side_effects=True, vmem_limit_bytes=61000 * 1024
        ),
        cost_estimate=pl.CostEstimate(
            flops=flops, bytes_accessed=8 * rows * width, transcendentals=0
        ),
    )(scal, images, ivalid, scaled, tmask)
    return (
        ig,
        tg.reshape(rows, width),
        jnp.sum(loss, axis=1),
        jnp.sum(sums.reshape(2, 8 * SPAN), axis=1),
    )


def solution(mesh):
    B, G = mesh.shape["blk"], mesh.shape["grp"]
    whole = P(("blk", "grp"), None)
    split = P(("blk", "grp"))
    return jax.shard_map(
        functools.partial(on_device, B, G),
        mesh=mesh,
        in_specs=(whole, whole, split, split, P(), P()),
        out_specs=(whole, whole, split, P()),
        check_vma=False,
    )
```

```python
import functools

import jax
import jax.numpy as jnp
from jax import lax
from jax.experimental import pallas as pl
from jax.experimental.pallas import tpu as pltpu
from jax.sharding import PartitionSpec as P

MESH = pl.DeviceIdType.MESH
SPAN = 128
F32 = jnp.float32
BF16 = jnp.bfloat16


def kernel(
    B, G, C, L,
    scal, img, txt, info,
    ig, igr, tg, loss, sums,
    T, A, RX, X, M, gacc, gsend, lsend, lrecv, acc, sz, sb,
    load_sem, agS, agR, rS, rR, mS, mR, iS, iR, kS, kR, szS, szR, sbS, sbR,
):
    b = lax.axis_index("blk")
    z = lax.axis_index("grp")
    rows = loss.shape[0]
    nxt = lax.rem(b + 1, B)
    prv = lax.rem(b + B - 1, B)
    up = jnp.minimum(z + 1, G - 1)
    down = jnp.maximum(z - 1, 0)
    temp = scal[0]
    bias = scal[1]

    def remote(src, dst, ss, rs, dev):
        return pltpu.make_async_remote_copy(
            src_ref=src, dst_ref=dst, send_sem=ss, recv_sem=rs, device_id=dev, device_id_type=MESH
        )

    loads = [
        pltpu.make_async_copy(txt, T.at[z], load_sem.at[0]),
        pltpu.make_async_copy(info, M.at[z], load_sem.at[1]),
        pltpu.make_async_copy(img, X.at[pl.ds(0, rows)], load_sem.at[2]),
    ]
    for load in loads:
        load.start()

    bar = pltpu.get_barrier_semaphore()
    for d in range(1, G):
        pl.semaphore_signal(bar, inc=1, device_id=(b, lax.rem(z + d, G)), device_id_type=MESH)
    for d in range(1, B):
        pl.semaphore_signal(bar, inc=1, device_id=(lax.rem(b + d, B), z), device_id_type=MESH)

    gacc[...] = jnp.zeros_like(gacc)
    loss[...] = jnp.zeros_like(loss)
    lsend[...] = jnp.zeros_like(lsend)
    acc[...] = jnp.zeros_like(acc)
    tg[...] = jnp.zeros_like(tg)
    for load in loads:
        load.wait()
    pl.semaphore_wait(bar, G + B - 2)

    def ag(zt, c, direction):
        return remote(T.at[zt, c], T.at[zt, c], agS.at[direction, zt, c], agR.at[zt, c],
                      (b, up if direction == 0 else down))

    def rs(zt, c, slot, direction):
        return remote(A.at[zt, c], RX.at[slot, c], rS.at[zt, c], rR.at[slot, c],
                      (b, up if direction == 0 else down))

    def info_z(d, place, other):
        return remote(info, M.at[place], mS.at[d], mR.at[place], (b, other))

    to_prev = [
        remote(X.at[pl.ds(0, rows)], X.at[pl.ds(rows, rows)], iS.at[0], iR.at[0], (prv, z)),
        remote(info, M.at[G], iS.at[1], iR.at[1], (prv, z)),
    ]
    to_next = [
        remote(gsend, igr, kS.at[0], kR.at[0], (nxt, z)),
        remote(lsend, lrecv, kS.at[1], kR.at[1], (nxt, z)),
    ]

    def item(t, kind):
        if kind == 2:
            start = max(C * (G - 1) - C - 1, 0)
            return (t >= start) & (t < start + C), jnp.clip(t - start, 0, C - 1), z
        n = G - 1 - z if kind == 0 else z
        safe = jnp.maximum(n, 1)
        j = t - 1
        valid = (j >= 0) & (j < C * n)
        j = jnp.clip(j, 0, C * safe - 1)
        c = lax.div(j, safe)
        off = 1 + lax.rem(j, safe)
        zt = z + off if kind == 0 else z - off
        return valid, c, jnp.clip(zt, 0, G - 1)

    def tile(zt, c):
        scale = M[zt, c + 1][0:1, 0:1]
        block = (T[zt, c].astype(F32) * scale).astype(BF16)
        text_count = M[zt, 0][0:1, :]
        col = lax.broadcasted_iota(jnp.int32, (rows, SPAN), 1) + c * SPAN
        row = lax.broadcasted_iota(jnp.int32, (rows, SPAN), 0)
        col_on = col.astype(F32) < text_count
        part = None
        for step in (0, 1):
            here = pl.ds(step * rows, rows)
            scores = lax.dot_general(
                X[here, :], block, (((1,), (1,)), ((), ())), preferred_element_type=F32
            )
            scaled = temp * scores
            logits = scaled + bias
            on = col_on & (row.astype(F32) < M[z if step == 0 else G, 0][0:1, :])
            if step == 0:
                match = col + (zt - z) * rows == row
                x = jnp.where(match, -logits, logits)
            else:
                x = logits
            e = jnp.exp(-jnp.abs(x))
            soft = jnp.maximum(x, 0.0) + jnp.log1p(e)
            dlogit = jnp.where(x >= 0, 1.0, e) / (1.0 + e)
            if step == 0:
                dlogit = jnp.where(match, -dlogit, dlogit)
            dlogit = jnp.where(on, dlogit, 0.0)
            total = loss if step == 0 else lsend
            total[...] += jnp.where(on, soft, 0.0)
            acc[0:8, :] += jnp.sum((dlogit * scaled).reshape(rows // 8, 8, SPAN), axis=0)
            acc[8:16, :] += jnp.sum(dlogit.reshape(rows // 8, 8, SPAN), axis=0)
            dround = dlogit.astype(BF16)
            gacc[here, :] += jnp.dot(dround, block, preferred_element_type=F32)
            piece = lax.dot_general(
                dround, X[here, :], (((0,), (0,)), ((), ())), preferred_element_type=F32
            )
            part = piece if part is None else part + piece
        return temp * part

    jobs_end = C * (G - 1) + 1
    slots = C * (G - 1) + G + L

    def slot(t, carry):
        for direction in (0, 1):
            n = z + 1 if direction == 0 else G - z
            c = lax.div(t, n)
            edge = z < G - 1 if direction == 0 else z > 0
            due = edge & (lax.rem(t, n) == 0) & (c < C)

            @pl.when(due)
            def _():
                ag(z, jnp.minimum(c, C - 1), direction).start()

        @pl.when(t == 0)
        def _():
            for copy in reversed(to_prev):
                copy.start()
            for d in range(1, G):
                info_z(d, z, lax.rem(z + d, G)).start()
            for d in range(1, G):
                other = lax.rem(z + d, G)
                info_z(d, other, other).wait_recv()

        for kind in (0, 1):
            valid, c, zt = item(t, kind)

            @pl.when(valid)
            def _():
                onward = 1 if kind == 0 else 0
                ag(zt, c, onward).wait_recv()

                @pl.when(z > 0 if kind == 0 else z < G - 1)
                def _():
                    ag(zt, c, onward).start()

        @pl.when(t == 1)
        def _():
            for copy in to_prev:
                copy.wait_recv()

        def job(kind, carry):
            v0, c0, z0 = item(t, 0)
            v1, c1, z1 = item(t, 1)
            v2, c2, z2 = item(t, 2)
            c = jnp.where(kind == 0, c0, jnp.where(kind == 1, c1, c2))
            zt = jnp.where(kind == 0, z0, jnp.where(kind == 1, z1, z2))
            valid = ((kind == 0) & v0) | ((kind == 1) & v1) | ((kind == 2) & v2)

            @pl.when(valid)
            def _():
                part = tile(zt, c)

                @pl.when(kind == 2)
                def _():
                    tg[c] += part

                @pl.when(kind != 2)
                def _():
                    A[zt, c] = part.astype(BF16)

            return carry

        @pl.when((t < jobs_end) & (t > 0))
        def _():
            lax.fori_loop(0, 3, job, 0)

        for direction in (0, 1):
            far = z if direction == 0 else G - 1 - z
            v = t - 1 - L - far
            vc = jnp.clip(v, 0, C * (G - 1) - 1)
            c = lax.div(vc, G - 1)
            target = lax.rem(vc, G - 1) + 1
            zt = target if direction == 0 else G - 1 - target
            live = (v >= 0) & (v < C * (G - 1)) & (target >= far)

            @pl.when(live & (target > far))
            def _():
                @pl.when(far > 0)
                def _():
                    rs(zt, c, zt, direction).wait_recv()
                    A[zt, c] = (A[zt, c].astype(F32) + RX[zt, c].astype(F32)).astype(BF16)

                last = target == far + 1
                where = jnp.where(last & (direction == 1), G, zt)
                rs(zt, c, where, direction).start()

            @pl.when(live & (target == far))
            def _():
                place = z if direction == 0 else G
                rs(zt, c, place, direction).wait_recv()
                tg[c] = tg[c] + RX[place, c].astype(F32)

        @pl.when(t == jobs_end - 1)
        def _():
            for d in range(1, G):
                remote(acc, sz.at[z], szS.at[d], szR.at[z], (b, lax.rem(z + d, G))).start()
            gsend[...] = (temp * gacc[pl.ds(rows, rows), :]).astype(BF16)
            to_next[1].start()
            to_next[0].start()
            sz[z] = acc[...]

        @pl.when(t == jobs_end)
        def _():
            ig[...] = temp * gacc[pl.ds(0, rows), :]
            for d in range(1, G):
                other = lax.rem(z + d, G)
                remote(acc, sz.at[other], szS.at[d], szR.at[other], (b, other)).wait_recv()
            total = sz[0]
            for g in range(1, G):
                total = total + sz[g]
            sz[G] = total
            sb[b] = total
            for d in range(1, B):
                remote(sz.at[G], sb.at[b], sbS.at[d], sbR.at[b], (lax.rem(b + d, B), z)).start()

        return carry

    lax.fori_loop(0, slots, slot, 0)

    for d in range(1, B):
        other = lax.rem(b + d, B)
        remote(sz.at[G], sb.at[other], sbS.at[d], sbR.at[other], (other, z)).wait_recv()
    total = sb[0]
    for g in range(1, B):
        total = total + sb[g]
    sums[...] = total
    for copy in to_next:
        copy.wait_recv()
    loss[...] += lrecv[...]

    for copy in to_prev + to_next:
        copy.wait_send()
    for d in range(1, G):
        other = lax.rem(z + d, G)
        info_z(d, z, other).wait_send()
        remote(acc, sz.at[z], szS.at[d], szR.at[z], (b, other)).wait_send()
    for d in range(1, B):
        remote(sz.at[G], sb.at[b], sbS.at[d], sbR.at[b], (lax.rem(b + d, B), z)).wait_send()

    def drain(i, carry):
        zt, c = lax.div(i, C), lax.rem(i, C)

        @pl.when(zt != z)
        def _():
            rs(zt, c, zt, 0).wait_send()

        @pl.when((zt <= z) & (z < G - 1))
        def _():
            ag(zt, c, 0).wait_send()

        @pl.when((zt >= z) & (z > 0))
        def _():
            ag(zt, c, 1).wait_send()

        return carry

    lax.fori_loop(0, G * C, drain, 0)


def on_device(B, G, images, texts, text_exps, counts, log_temp, bias):
    rows, width = images.shape
    C = rows // SPAN
    scale = jnp.exp2(text_exps.astype(F32))
    scal = jnp.concatenate([jnp.exp(log_temp), bias])
    info = jnp.broadcast_to(
        jnp.concatenate([counts.astype(F32), scale])[:, None, None], (C + 1, 8, SPAN)
    )
    vmem = pl.BlockSpec(memory_space=pltpu.VMEM)
    hbm = pl.BlockSpec(memory_space=pl.ANY)
    dma = pltpu.SemaphoreType.DMA
    flops = 2 * G * 3 * 2 * rows * rows * width
    ig, igr, tg, loss, sums = pl.pallas_call(
        functools.partial(kernel, B, G, C, 0),
        out_shape=(
            jax.ShapeDtypeStruct((rows, width), F32),
            jax.ShapeDtypeStruct((rows, width), BF16),
            jax.ShapeDtypeStruct((C, SPAN, width), F32),
            jax.ShapeDtypeStruct((rows, SPAN), F32),
            jax.ShapeDtypeStruct((16, SPAN), F32),
        ),
        in_specs=[pl.BlockSpec(memory_space=pltpu.SMEM), hbm, hbm, vmem],
        out_specs=(vmem, vmem, vmem, vmem, vmem),
        scratch_shapes=[
            pltpu.VMEM((G, C, SPAN, width), BF16),
            pltpu.VMEM((G, C, SPAN, width), BF16),
            pltpu.VMEM((G + 1, C, SPAN, width), BF16),
            pltpu.VMEM((2 * rows, width), BF16),
            pltpu.VMEM((G + 1, C + 1, 8, SPAN), F32),
            pltpu.VMEM((2 * rows, width), F32),
            pltpu.VMEM((rows, width), BF16),
            pltpu.VMEM((rows, SPAN), F32),
            pltpu.VMEM((rows, SPAN), F32),
            pltpu.VMEM((16, SPAN), F32),
            pltpu.VMEM((G + 1, 16, SPAN), F32),
            pltpu.VMEM((B, 16, SPAN), F32),
            dma((3,)),
            dma((2, G, C)), dma((G, C)),
            dma((G, C)), dma((G + 1, C)),
            dma((G,)), dma((G,)),
            dma((2,)), dma((2,)),
            dma((2,)), dma((2,)),
            dma((G,)), dma((G,)),
            dma((B,)), dma((B,)),
        ],
        compiler_params=pltpu.CompilerParams(
            collective_id=0, has_side_effects=True, vmem_limit_bytes=61000 * 1024
        ),
        cost_estimate=pl.CostEstimate(
            flops=flops, bytes_accessed=8 * rows * width, transcendentals=0
        ),
    )(scal, images, texts.reshape(C, SPAN, width), info)
    return (
        ig + igr.astype(F32),
        tg.reshape(rows, width),
        jnp.sum(loss, axis=1),
        jnp.sum(sums.reshape(2, 8 * SPAN), axis=1),
    )


def solution(mesh):
    B, G = mesh.shape["blk"], mesh.shape["grp"]
    whole = P(("blk", "grp"), None)
    split = P(("blk", "grp"))
    return jax.shard_map(
        functools.partial(on_device, B, G),
        mesh=mesh,
        in_specs=(whole, whole, split, split, P(), P()),
        out_specs=(whole, whole, split, P()),
        check_vma=False,
    )
```
